32 devices in a mesh: task: 4 (over z), mp: 8 (over y, x, core).
Axes of the slice: x: 2, y: 2, z: 4, core: 2. Of those that a mesh axis runs over, the one named last changes fastest.
Arguments:
- deter: float32 [1024, 4096], P('task', 'mp'), may hold values from -3 to 3
- draws: int32 [4, 32, 1024], P(None, None, 'task'), may hold values from 0 to 31
- actions: int32 [4, 1024], P(None, 'task'), may hold values from 0 to 17
- horizons: int32 [64], replicated, may hold values from 5 to 30, as said below
- offsets: int32 [4, 4], replicated, may hold values from 0 to 3, as said below
- embed_stoch: bfloat16 [1024, 1024], replicated, may hold values from -1 to 1
- embed_act: bfloat16 [18, 1024], replicated, may hold values from -6 to 6
- gru_weight: bfloat16 [5120, 3, 4096], P(None, None, 'mp'), may hold values from -0.078125 to 0.078125
- prior_weight: bfloat16 [4096, 1024], replicated, may hold values from -0.09375 to 0.09375
- logit_weight: bfloat16 [1024, 1024], replicated, may hold values from -0.75 to 0.75
- head_weight: bfloat16 [1024, 2], replicated, may hold values from -0.375 to 0.375
Outputs:
- log_prob: float32 [4, 1024], P(None, 'task')
- reward: float32 [4, 1024], P(None, 'task')
- continuation: float32 [4, 1024], P(None, 'task')
- final_deter: float32 [1024, 4096], P('task', 'mp')
The draws below stay inside these ranges and needn't reach their ends.
Inputs may be any that keep to these rules, and one draw needn't show every extreme that they name: `horizons`: rows of task k are home rows k * (16) up to (k + 1) * 16 - 1. `offsets`: the 4 numbers of one row are distinct.
All inputs are finite; a program needn't handle non-finite values.
Results may differ from the reference program's by a relative error of at most 0.0045.
Values may be sent and summed in bfloat16 or wider, within the bound.
A program may use at most 128 MiB of HBM per device.

```python
import jax
import jax.numpy as jnp
from jax import lax

DET = 4096
HID = 1024
GROUPS = 32
CLASSES = 32
ACTS = 18
TASKS = 64
BLK_DEV = 4
BROWS = 64
STEPS = 4
WSTART = 16
STOCH = 1024
BLOCKS = 16
ROWS = 1024
N_TASK = 4


def plan_helper(key):
    horizon_key = jax.random.fold_in(key, 11)
    horizons = jax.random.randint(horizon_key, (TASKS,), 5, 31).astype(jnp.int32)
    holders = BLOCKS // BLK_DEV
    per_task = BLOCKS * BROWS // TASKS
    row_task = jnp.arange(BLOCKS * BROWS, dtype=jnp.int32) // per_task
    places = jnp.arange(holders, dtype=jnp.int32)[:, None]
    local_slot = jnp.arange(BLK_DEV, dtype=jnp.int32)[None, :]
    running = jnp.zeros((BLK_DEV,), jnp.int32)
    shift_rows = []
    for moment in range(STEPS):
        live_rows = (horizons[row_task] > WSTART + moment).astype(jnp.int32)
        live_blocks = jnp.max(live_rows.reshape(BLOCKS, BROWS), axis=1).reshape(holders, BLK_DEV)
        moment_key = jax.random.fold_in(jax.random.fold_in(key, 23), moment)
        candidates = []
        heaviest = []
        for option in range(16):
            shifts = jax.random.permutation(jax.random.fold_in(moment_key, option), holders)[:BLK_DEV].astype(jnp.int32)
            landing = (running + shifts) % holders
            source = (places - landing[None, :]) % holders
            slot_live = live_blocks[source, local_slot]
            heaviest.append(jnp.max(jnp.sum(slot_live, axis=1)))
            candidates.append(shifts)
        chosen = jnp.argmin(jnp.stack(heaviest))
        shifts = jnp.stack(candidates)[chosen]
        running = (running + shifts) % holders
        shift_rows.append(shifts)
    return (horizons, jnp.stack(shift_rows).astype(jnp.int32))


def draw_horizons(key, part):
    return plan_helper(key)[0]


def draw_offsets(key, part):
    return plan_helper(key)[1]


def set_ends(array, stream_key, smallest, high):
    shape = array.shape
    index_at = [jax.random.randint(jax.random.fold_in(stream_key, axis), (), 0, shape[axis]) for axis in range(len(shape))]
    array = array.at[tuple(index_at)].set(smallest)
    longest = shape.index(max(shape))
    index_at[longest] = (index_at[longest] + 1) % shape[longest]
    return array.at[tuple(index_at)].set(high)


def level_of(stream_key, dims, pieces, smallest, high):
    factor_of = 1.0
    for axis_at, blocks in pieces:
        steps = jax.random.uniform(jax.random.fold_in(jax.random.fold_in(stream_key, 6), axis_at), (blocks,), jnp.float32, smallest / len(pieces), high / len(pieces))
        factor_of = factor_of * jnp.repeat(jnp.exp(steps), dims[axis_at] // blocks).reshape((-1,) + (1,) * (len(dims) - 1 - axis_at))
    return factor_of


def normal_values(stream_key, shape, deviation, limit, cuts=(), held_as=jnp.bfloat16):
    factor_of = level_of(stream_key, shape, cuts, -0.22, 0.18) if cuts else 1.0
    values = jax.random.normal(stream_key, shape, jnp.float32) * deviation * factor_of
    return jnp.minimum(jnp.maximum(values, -limit), limit).astype(held_as)


def setup_inputs(seed: int = 0) -> dict:
    arg_keys = jax.random.split(jax.random.key(seed), 12)
    deter = normal_values(arg_keys[0], (ROWS, DET), 0.5, 3.0, ((0, 4), (1, 8)), jnp.float32)
    draws = set_ends(jax.random.randint(arg_keys[1], (STEPS, GROUPS, ROWS), 0, CLASSES), jax.random.fold_in(arg_keys[1], 1), 0, CLASSES - 1).astype(jnp.int32)
    actions = set_ends(jax.random.randint(arg_keys[2], (STEPS, ROWS), 0, ACTS), jax.random.fold_in(arg_keys[2], 1), 0, ACTS - 1).astype(jnp.int32)
    horizons = draw_horizons(jax.random.fold_in(arg_keys[11], 71), 0)
    offsets = draw_offsets(jax.random.fold_in(arg_keys[11], 71), 0)
    embed_stoch = normal_values(arg_keys[5], (STOCH, HID), GROUPS ** -0.5, 1.0)
    embed_act = normal_values(arg_keys[6], (ACTS, HID), 1.0, 6.0)
    gru_weight = normal_values(arg_keys[7], (HID + DET, 3, DET), (HID + DET) ** -0.5, 0.078125, ((2, 8),))
    prior_weight = normal_values(arg_keys[8], (DET, HID), DET ** -0.5, 0.09375)
    logit_weight = normal_values(arg_keys[9], (HID, STOCH), (HID // 16) ** -0.5, 0.75)
    head_weight = normal_values(arg_keys[10], (HID, 2), (HID // 4) ** -0.5, 0.375)
    return {"deter": deter, "draws": draws, "actions": actions, "horizons": horizons, "offsets": offsets, "embed_stoch": embed_stoch, "embed_act": embed_act, "gru_weight": gru_weight, "prior_weight": prior_weight, "logit_weight": logit_weight, "head_weight": head_weight}


def layer_norm(values):
    average = lax.optimization_barrier(jnp.mean(values, axis=-1, keepdims=True))
    squares = lax.optimization_barrier(jnp.mean(values * values, axis=-1, keepdims=True))
    return (values - average) * lax.rsqrt(squares - average * average + 1e-05)

def reference(deter, draws, actions, horizons, offsets, embed_stoch, embed_act, gru_weight, prior_weight, logit_weight, head_weight):
    rows_total = deter.shape[0]
    per_task = rows_total // TASKS
    holders = N_TASK
    places = jnp.arange(holders, dtype=jnp.int32)[:, None]
    local_slot = jnp.arange(BLK_DEV, dtype=jnp.int32)[None, :]
    within = jnp.arange(BROWS, dtype=jnp.int32)
    classes = jnp.arange(CLASSES, dtype=jnp.int32)
    action_ids = jnp.arange(ACTS, dtype=jnp.int32)
    gate_matrix = gru_weight.reshape(HID + DET, 3 * DET)
    carried = deter
    running = jnp.zeros((BLK_DEV,), jnp.int32)
    logp_list, reward_list, cont_list = ([], [], [])
    for moment in range(STEPS):
        offset_now = offsets[moment].astype(jnp.int32)
        source = ((places - offset_now[None, :]) % holders).astype(jnp.int32)
        carried = carried.reshape(holders, BLK_DEV, BROWS, DET)[source, local_slot].reshape(rows_total, DET)
        running = (running + offset_now) % holders
        home_block = (places - running[None, :]) % holders * BLK_DEV + local_slot
        home_rows = (home_block[:, :, None] * BROWS + within).reshape(rows_total).astype(jnp.int32)
        living = (horizons[home_rows // per_task] > WSTART + moment).astype(jnp.float32)
        chosen_hot = (jnp.transpose(draws[moment])[:, :, None] == classes).astype(jnp.float32)
        stoch_hot = chosen_hot.astype(jnp.bfloat16).reshape(rows_total, STOCH)
        action_hot = (actions[moment][:, None] == action_ids[None, :]).astype(jnp.bfloat16)
        carried_low = carried.astype(jnp.bfloat16)
        embed_pre = jnp.dot(stoch_hot, embed_stoch, preferred_element_type=jnp.float32) + jnp.dot(action_hot, embed_act, preferred_element_type=jnp.float32)
        embedded = jax.nn.silu(layer_norm(embed_pre)).astype(jnp.bfloat16)
        joined = jnp.concatenate([embedded, carried_low], axis=1)
        gate_parts = jnp.dot(joined, gate_matrix, preferred_element_type=jnp.float32)
        normed = layer_norm(gate_parts).reshape(rows_total, 3, DET)
        reset_gate = jax.nn.sigmoid(normed[:, 0])
        candidate = jnp.tanh(reset_gate * normed[:, 1])
        update = jax.nn.sigmoid(normed[:, 2] - 1.0)
        renewed = update * candidate + (1.0 - update) * carried
        prior_pre = jnp.dot(carried_low, prior_weight, preferred_element_type=jnp.float32)
        hidden = jax.nn.silu(layer_norm(prior_pre)).astype(jnp.bfloat16)
        raw_logits = jnp.dot(hidden, logit_weight, preferred_element_type=jnp.float32).reshape(rows_total, GROUPS, CLASSES)
        capped = 5.0 * jnp.tanh(raw_logits / 5.0)
        exponent = jnp.exp(capped)
        chances = 0.99 * exponent / lax.optimization_barrier(jnp.sum(exponent, axis=-1, keepdims=True)) + 0.01 / CLASSES
        log_prob = lax.optimization_barrier(jnp.sum(jnp.log(lax.optimization_barrier(jnp.sum(chances * chosen_hot, axis=-1))), axis=-1)) * living
        head_out = jnp.dot(hidden, head_weight, preferred_element_type=jnp.float32)
        logp_list.append(log_prob)
        reward_list.append(head_out[:, 0] * living)
        cont_list.append(jax.nn.sigmoid(head_out[:, 1]) * living)
        carried = jnp.where(living[:, None] > 0, renewed, carried)
    return (jnp.stack(logp_list), jnp.stack(reward_list), jnp.stack(cont_list), carried)
```

```python
import jax
import jax.numpy as jnp
from jax import lax
from jax.sharding import PartitionSpec as P

HID = 1024
GROUPS = 32
CLASSES = 32
ACTS = 18
TASKS = 64
BLK_DEV = 4
STEPS = 4
WSTART = 16


def normed_rows(values):
    entries = values.shape[-1]
    average = jnp.sum(values, axis=-1, keepdims=True) / entries
    squares = jnp.sum(values * values, axis=-1, keepdims=True) / entries
    return (values - average) * lax.rsqrt(squares - average * average + 1e-05)


def product(rows_in, weight):
    return jnp.dot(rows_in, weight, preferred_element_type=jnp.float32)


def recurrence(deter, embedded, gate_weight, living, det_full):
    carried = deter
    rows_here, det_share = deter.shape
    lows = []
    for moment in range(STEPS):
        low = carried.astype(jnp.bfloat16)
        gathered = lax.all_gather(low, "mp", axis=1, tiled=True)
        lows.append(gathered)
        joined = jnp.concatenate([embedded[moment], gathered], axis=1)
        parts = [product(joined, gate_weight[part]) for part in range(3)]
        sums = sum(jnp.sum(part, axis=1) for part in parts)
        squares = sum(jnp.sum(part * part, axis=1) for part in parts)
        sums, squares = lax.psum(jnp.stack([sums, squares]), "mp")
        average = sums / (3 * det_full)
        inverse = lax.rsqrt(squares / (3 * det_full) - average * average + 1e-05)
        normed = [(part - average[:, None]) * inverse[:, None] for part in parts]
        reset_gate = jax.nn.sigmoid(normed[0])
        candidate = jnp.tanh(reset_gate * normed[1])
        update = jax.nn.sigmoid(normed[2] - 1.0)
        renewed = update * candidate + (1.0 - update) * carried
        carried = jnp.where(living[moment][:, None] > 0, renewed, carried)
    return carried, lows


def on_device(
    deter,
    draws,
    actions,
    horizons,
    offsets,
    embed_stoch,
    embed_act,
    gru_weight,
    prior_weight,
    logit_weight,
    head_weight,
):
    holders = lax.axis_size("task")
    device = lax.axis_index("task")
    shards = lax.axis_size("mp")
    shard_index = lax.axis_index("mp")
    rows_here, det_share = deter.shape
    block_rows = rows_here // BLK_DEV
    per_task = rows_here * holders // TASKS
    own_rows = rows_here // shards
    places = jnp.arange(holders, dtype=jnp.int32)
    classes = jnp.arange(CLASSES, dtype=jnp.int32)
    running = jnp.cumsum(offsets, axis=0) % holders
    packed = jnp.concatenate([draws, actions[:, None]], axis=1).astype(jnp.bfloat16)
    packed = lax.all_gather(packed, "task")
    packed = packed.reshape(holders, STEPS, GROUPS + 1, BLK_DEV, block_rows)
    at_slot = (device + running) % holders
    picked = places[:, None, None] == at_slot[None]
    packed = jnp.sum(
        jnp.where(picked[:, :, None, :, None], packed.astype(jnp.float32), 0.0), axis=0
    ).astype(jnp.int32)
    packed = packed.reshape(STEPS, GROUPS + 1, rows_here)
    draws_home = jnp.transpose(packed[:, :GROUPS], (0, 2, 1))
    hot = (draws_home[:, :, :, None] == classes).astype(jnp.bfloat16)
    hot = hot.reshape(STEPS * rows_here, GROUPS * CLASSES)
    action_hot = (
        packed[:, GROUPS].reshape(-1)[:, None] == jnp.arange(ACTS, dtype=jnp.int32)
    ).astype(jnp.bfloat16)
    embed_pre = product(hot, embed_stoch) + product(action_hot, embed_act)
    embedded = jax.nn.silu(normed_rows(embed_pre)).astype(jnp.bfloat16)
    embedded = embedded.reshape(STEPS, rows_here, HID)

    home_rows = device * rows_here + jnp.arange(rows_here, dtype=jnp.int32)
    task_ids = jnp.arange(TASKS, dtype=jnp.int32)
    horizon_rows = jnp.sum(
        jnp.where((home_rows // per_task)[:, None] == task_ids, horizons, 0), axis=1
    )
    alive = horizon_rows[None] > WSTART + jnp.arange(STEPS, dtype=jnp.int32)[:, None]
    living = alive.astype(jnp.float32)

    gate_weight = jnp.transpose(gru_weight, (1, 0, 2))
    carried, lows = recurrence(deter, embedded, gate_weight, living, det_share * shards)

    target = (device + running[-1]) % holders
    sending = places[:, None] == target[None, :]
    blocks = carried.reshape(BLK_DEV, block_rows, det_share)
    outgoing = jnp.where(sending[:, :, None, None], blocks[None], 0.0).astype(jnp.bfloat16)
    arrived = lax.all_to_all(
        outgoing.reshape(holders * BLK_DEV * block_rows, det_share),
        "task",
        split_axis=0,
        concat_axis=0,
        tiled=True,
    ).reshape(holders, BLK_DEV, block_rows, det_share)
    taking = places[:, None] == ((device - running[-1]) % holders)[None, :]
    final = jnp.sum(
        jnp.where(taking[:, :, None, None], arrived.astype(jnp.float32), 0.0), axis=0
    ).reshape(rows_here, det_share)

    def own(array, axis):
        return lax.dynamic_slice_in_dim(array, shard_index * own_rows, own_rows, axis)

    state_rows = jnp.concatenate([own(low, 0) for low in lows], axis=0)
    hidden = jax.nn.silu(normed_rows(product(state_rows, prior_weight))).astype(jnp.bfloat16)
    raw = product(hidden, logit_weight).reshape(STEPS * own_rows, GROUPS, CLASSES)
    exponent = jnp.exp(5.0 * jnp.tanh(raw / 5.0))
    own_hot = own(draws_home, 1).reshape(STEPS * own_rows, GROUPS)[:, :, None] == classes
    chosen = jnp.sum(jnp.where(own_hot, exponent, 0.0), axis=-1)
    chances = 0.99 * chosen / jnp.sum(exponent, axis=-1) + 0.01 / CLASSES
    log_prob = jnp.sum(jnp.log(chances), axis=-1)
    head_out = product(hidden, head_weight)
    results = jnp.stack([log_prob, head_out[:, 0], jax.nn.sigmoid(head_out[:, 1])])
    results = results.reshape(3, STEPS, own_rows) * own(living, 1)[None]
    spread = lax.all_gather(results, ("task", "mp"))
    spread = spread.reshape(holders, shards, 3, STEPS, own_rows)
    spread = jnp.transpose(spread, (0, 2, 3, 1, 4)).reshape(
        holders, 3, STEPS, BLK_DEV, block_rows
    )
    source = (device - running) % holders
    from_home = places[:, None, None] == source[None]
    outs = jnp.sum(jnp.where(from_home[:, None, :, :, None], spread, 0.0), axis=0)
    outs = outs.reshape(3, STEPS, rows_here)
    return (outs[0], outs[1], outs[2], final)


def solution(mesh):
    in_specs = (
        P("task", "mp"),
        P(None, None, "task"),
        P(None, "task"),
        P(),
        P(),
        P(),
        P(),
        P(None, None, "mp"),
        P(),
        P(),
        P(),
    )
    out_specs = (P(None, "task"), P(None, "task"), P(None, "task"), P("task", "mp"))
    return jax.shard_map(
        on_device, mesh=mesh, in_specs=in_specs, out_specs=out_specs, check_vma=False
    )
```

```python
import functools

import jax
import jax.numpy as jnp
from jax import lax
from jax.experimental import pallas as pl
from jax.experimental.pallas import tpu as pltpu
from jax.sharding import PartitionSpec as P

HID = 1024
GROUPS = 32
CLASSES = 32
ACTS = 18
TASKS = 64
BLK_DEV = 4
STEPS = 4
WSTART = 16


def normed_rows(values):
    entries = values.shape[-1]
    average = jnp.sum(values, axis=-1, keepdims=True) / entries
    squares = jnp.sum(values * values, axis=-1, keepdims=True) / entries
    return (values - average) * lax.rsqrt(squares - average * average + 1e-05)


def product(rows_in, weight):
    return jnp.dot(rows_in, weight, preferred_element_type=jnp.float32)


def flipped(index, mask):
    bit = 1
    while bit <= mask:
        if mask & bit:
            index = index + bit * (1 - 2 * ((index // bit) % 2))
        bit *= 2
    return index


def window_kernel(
    shards,
    groups,
    rows,
    share,
    deter_ref,
    embedded_ref,
    living_ref,
    weight_ref,
    carried_ref,
    lows_ref,
    weight,
    gath,
    parts,
    stats,
    weight_sem,
    low_sem,
    send_sem,
    recv_sem,
    stat_send,
    stat_recv,
):
    me = lax.axis_index("mp")
    peers = {mask: flipped(me, mask) for mask in range(1, shards)}
    fetch = pltpu.make_async_copy(weight_ref, weight, weight_sem)
    fetch.start()
    barrier = pltpu.get_barrier_semaphore()
    for mask in range(1, shards):
        pl.semaphore_signal(
            barrier,
            inc=1,
            device_id={"mp": peers[mask]},
            device_id_type=pl.DeviceIdType.MESH,
        )
    bits = []
    bit = shards // 2
    while bit:
        bits.append(bit)
        bit //= 2
    orders = [bits, [bits[1], bits[0]] + bits[2:]]
    half = rows // 2
    masks = sorted(range(1, shards), key=lambda mask: (mask.bit_count(), mask))

    def source(mask):
        return me if mask == 0 else peers[mask]

    def hop(g, s, mask, via):
        block = gath.at[g, source(mask), pl.ds(s * half, half)]
        return pltpu.make_async_remote_copy(
            src_ref=block,
            dst_ref=block,
            send_sem=send_sem.at[g, s, mask ^ via],
            recv_sem=recv_sem.at[g, s, mask ^ via],
            device_id={"mp": peers[via]},
            device_id_type=pl.DeviceIdType.MESH,
        )

    def forward(g, s, mask):
        order = orders[s]
        last = max([order.index(bit) for bit in order if mask & bit], default=-1)
        for via in order[last + 1 :]:
            hop(g, s, mask, via).start()

    def arriving(g, s, mask):
        block = gath.at[g, source(mask), pl.ds(s * half, half)]
        return pltpu.make_async_remote_copy(
            src_ref=block,
            dst_ref=block,
            send_sem=send_sem.at[g, s, mask],
            recv_sem=recv_sem.at[g, s, mask],
            device_id={"mp": peers[mask]},
            device_id_type=pl.DeviceIdType.MESH,
        )

    def launch(g):
        here = pl.ds(g * rows, rows)
        gath[g, me] = carried_ref[here, :].astype(jnp.bfloat16)
        for s in range(2):
            forward(g, s, 0)

    def stat_copy(g, mask):
        return pltpu.make_async_remote_copy(
            src_ref=stats.at[g, 0],
            dst_ref=stats.at[g, mask],
            send_sem=stat_send.at[g, mask],
            recv_sem=stat_recv.at[g, mask],
            device_id={"mp": peers[mask]},
            device_id_type=pl.DeviceIdType.MESH,
        )

    def multiply(g, rows_in, start, depth, first):
        for part in range(3):
            term = jnp.dot(
                rows_in, weight[part, pl.ds(start, depth), :], preferred_element_type=jnp.float32
            )
            if first:
                parts[g, part] = term
            else:
                parts[g, part] += term

    carried_ref[...] = deter_ref[...]
    pl.semaphore_wait(barrier, shards - 1)
    for g in range(groups):
        launch(g)
    fetch.wait()

    def step(t, _):
        for g in range(groups):
            seen = set()

            def need(s, mask):
                if (s, mask) not in seen:
                    seen.add((s, mask))
                    arriving(g, s, mask).wait_recv()
                    forward(g, s, mask)

            multiply(g, embedded_ref[t, pl.ds(g * rows, rows), :], 0, HID, True)
            for s in range(2):
                need(s, orders[s][0])
            for mask in [0] + masks:
                if mask:
                    for s in range(2):
                        need(s, mask)
                start = pl.multiple_of(HID + source(mask) * share, share)
                multiply(g, gath[g, source(mask)], start, share, False)
            keep = pltpu.make_async_copy(gath.at[g], lows_ref.at[t, g], low_sem)
            keep.start()
            sums = jnp.zeros((rows, 128), jnp.float32)
            squares = jnp.zeros((rows, 128), jnp.float32)
            for part in range(3):
                for column in range(0, share, 128):
                    piece = parts[g, part, :, pl.ds(column, 128)]
                    sums = sums + piece
                    squares = squares + piece * piece
            stats[g, 0, 0:1, :] = jnp.sum(sums.T, axis=0, keepdims=True)
            stats[g, 0, 1:2, :] = jnp.sum(squares.T, axis=0, keepdims=True)
            for s in range(2):
                for mask in masks:
                    arriving(g, s, mask).wait_send()
            keep.wait()
            for mask in masks:
                stat_copy(g, mask).start()
        for g in range(groups):
            for mask in masks:
                stat_copy(g, mask).wait()
            total = jnp.sum(stats[g], axis=0) / (3 * share * shards)
            average = jnp.broadcast_to(total[0:1], (128, rows)).T
            square = jnp.broadcast_to(total[1:2], (128, rows)).T
            inverse = lax.rsqrt(square - average * average + 1e-05)
            here = pl.ds(g * rows, rows)
            alive = living_ref[t, here, :]
            for column in range(0, share, 128):
                where = pl.ds(column, 128)
                normed = [(parts[g, part, :, where] - average) * inverse for part in range(3)]
                reset_gate = jax.nn.sigmoid(normed[0])
                candidate = jnp.tanh(reset_gate * normed[1])
                update = jax.nn.sigmoid(normed[2] - 1.0)
                before = carried_ref[here, where]
                renewed = update * candidate + (1.0 - update) * before
                carried_ref[here, where] = jnp.where(alive > 0, renewed, before)

            @pl.when(t < STEPS - 1)
            def _():
                launch(g)

        return 0

    lax.fori_loop(0, STEPS, step, 0)


def recurrence(deter, embedded, gate_weight, living, shards):
    rows_here, share = deter.shape
    groups = 2
    rows = rows_here // groups
    alive = jnp.broadcast_to(living[:, :, None], (STEPS, rows_here, 128))
    vmem = pl.BlockSpec(memory_space=pltpu.VMEM)
    hbm = pl.BlockSpec(memory_space=pl.ANY)
    dma = pltpu.SemaphoreType.DMA
    return pl.pallas_call(
        functools.partial(window_kernel, shards, groups, rows, share),
        out_shape=(
            jax.ShapeDtypeStruct((rows_here, share), jnp.float32),
            jax.ShapeDtypeStruct((STEPS, groups, shards, rows, share), jnp.bfloat16),
        ),
        in_specs=[vmem, vmem, vmem, hbm],
        out_specs=(vmem, hbm),
        scratch_shapes=[
            pltpu.VMEM(gate_weight.shape, jnp.bfloat16),
            pltpu.VMEM((groups, shards, rows, share), jnp.bfloat16),
            pltpu.VMEM((groups, 3, rows, share), jnp.float32),
            pltpu.VMEM((groups, shards, 2, rows), jnp.float32),
            dma,
            dma,
            dma((groups, 2, shards)),
            dma((groups, 2, shards)),
            dma((groups, shards)),
            dma((groups, shards)),
        ],
        compiler_params=pltpu.CompilerParams(
            collective_id=0, has_side_effects=True, vmem_limit_bytes=48 * 1024 * 1024
        ),
    )(deter, embedded, alive, gate_weight)


def on_device(
    deter,
    draws,
    actions,
    horizons,
    offsets,
    embed_stoch,
    embed_act,
    gru_weight,
    prior_weight,
    logit_weight,
    head_weight,
):
    holders = lax.axis_size("task")
    device = lax.axis_index("task")
    shards = lax.axis_size("mp")
    shard_index = lax.axis_index("mp")
    rows_here, det_share = deter.shape
    block_rows = rows_here // BLK_DEV
    per_task = rows_here * holders // TASKS
    own_rows = rows_here // shards
    places = jnp.arange(holders, dtype=jnp.int32)
    classes = jnp.arange(CLASSES, dtype=jnp.int32)
    running = jnp.cumsum(offsets, axis=0) % holders
    packed = jnp.concatenate([draws, actions[:, None]], axis=1).astype(jnp.bfloat16)
    packed = lax.all_gather(packed, "task")
    packed = packed.reshape(holders, STEPS, GROUPS + 1, BLK_DEV, block_rows)
    at_slot = (device + running) % holders
    picked = places[:, None, None] == at_slot[None]
    packed = jnp.sum(
        jnp.where(picked[:, :, None, :, None], packed.astype(jnp.float32), 0.0), axis=0
    ).astype(jnp.int32)
    packed = packed.reshape(STEPS, GROUPS + 1, rows_here)
    draws_home = jnp.transpose(packed[:, :GROUPS], (0, 2, 1))
    hot = (draws_home[:, :, :, None] == classes).astype(jnp.bfloat16)
    hot = hot.reshape(STEPS * rows_here, GROUPS * CLASSES)
    action_hot = (
        packed[:, GROUPS].reshape(-1)[:, None] == jnp.arange(ACTS, dtype=jnp.int32)
    ).astype(jnp.bfloat16)
    embed_pre = product(hot, embed_stoch) + product(action_hot, embed_act)
    embedded = jax.nn.silu(normed_rows(embed_pre)).astype(jnp.bfloat16)
    embedded = embedded.reshape(STEPS, rows_here, HID)

    home_rows = device * rows_here + jnp.arange(rows_here, dtype=jnp.int32)
    task_ids = jnp.arange(TASKS, dtype=jnp.int32)
    horizon_rows = jnp.sum(
        jnp.where((home_rows // per_task)[:, None] == task_ids, horizons, 0), axis=1
    )
    alive = horizon_rows[None] > WSTART + jnp.arange(STEPS, dtype=jnp.int32)[:, None]
    living = alive.astype(jnp.float32)

    gate_weight = jnp.transpose(gru_weight, (1, 0, 2))
    carried, lows = recurrence(deter, embedded, gate_weight, living, shards)

    target = (device + running[-1]) % holders
    sending = places[:, None] == target[None, :]
    blocks = carried.reshape(BLK_DEV, block_rows, det_share)
    outgoing = jnp.where(sending[:, :, None, None], blocks[None], 0.0).astype(jnp.bfloat16)
    arrived = lax.all_to_all(
        outgoing.reshape(holders * BLK_DEV * block_rows, det_share),
        "task",
        split_axis=0,
        concat_axis=0,
        tiled=True,
    ).reshape(holders, BLK_DEV, block_rows, det_share)
    taking = places[:, None] == ((device - running[-1]) % holders)[None, :]
    final = jnp.sum(
        jnp.where(taking[:, :, None, None], arrived.astype(jnp.float32), 0.0), axis=0
    ).reshape(rows_here, det_share)

    def own(array, axis):
        return lax.dynamic_slice_in_dim(array, shard_index * own_rows, own_rows, axis)

    first = shard_index * own_rows
    group_rows = lows.shape[3]
    state_rows = lax.dynamic_slice(
        lows,
        (0, first // group_rows, 0, first % group_rows, 0),
        (STEPS, 1, shards, own_rows, det_share),
    )
    state_rows = jnp.transpose(state_rows, (0, 1, 3, 2, 4)).reshape(STEPS * own_rows, -1)
    hidden = jax.nn.silu(normed_rows(product(state_rows, prior_weight))).astype(jnp.bfloat16)
    raw = product(hidden, logit_weight).reshape(STEPS * own_rows, GROUPS, CLASSES)
    exponent = jnp.exp(5.0 * jnp.tanh(raw / 5.0))
    own_hot = own(draws_home, 1).reshape(STEPS * own_rows, GROUPS)[:, :, None] == classes
    chosen = jnp.sum(jnp.where(own_hot, exponent, 0.0), axis=-1)
    chances = 0.99 * chosen / jnp.sum(exponent, axis=-1) + 0.01 / CLASSES
    log_prob = jnp.sum(jnp.log(chances), axis=-1)
    head_out = product(hidden, head_weight)
    results = jnp.stack([log_prob, head_out[:, 0], jax.nn.sigmoid(head_out[:, 1])])
    results = results.reshape(3, STEPS, own_rows) * own(living, 1)[None]
    spread = lax.all_gather(results, ("task", "mp"))
    spread = spread.reshape(holders, shards, 3, STEPS, own_rows)
    spread = jnp.transpose(spread, (0, 2, 3, 1, 4)).reshape(
        holders, 3, STEPS, BLK_DEV, block_rows
    )
    source = (device - running) % holders
    from_home = places[:, None, None] == source[None]
    outs = jnp.sum(jnp.where(from_home[:, None, :, :, None], spread, 0.0), axis=0)
    outs = outs.reshape(3, STEPS, rows_here)
    return (outs[0], outs[1], outs[2], final)


def solution(mesh):
    in_specs = (
        P("task", "mp"),
        P(None, None, "task"),
        P(None, "task"),
        P(),
        P(),
        P(),
        P(),
        P(None, None, "mp"),
        P(),
        P(),
        P(),
    )
    out_specs = (P(None, "task"), P(None, "task"), P(None, "task"), P("task", "mp"))
    return jax.shard_map(
        on_device, mesh=mesh, in_specs=in_specs, out_specs=out_specs, check_vma=False
    )
```

```python
import functools

import jax
import jax.numpy as jnp
from jax import lax
from jax.experimental import pallas as pl
from jax.experimental.pallas import tpu as pltpu
from jax.sharding import PartitionSpec as P

HID = 1024
GROUPS = 32
CLASSES = 32
ACTS = 18
TASKS = 64
BLK_DEV = 4
STEPS = 4
WSTART = 16


def normed_rows(values):
    entries = values.shape[-1]
    average = jnp.sum(values, axis=-1, keepdims=True) / entries
    squares = jnp.sum(values * values, axis=-1, keepdims=True) / entries
    return (values - average) * lax.rsqrt(squares - average * average + 1e-05)


def product(rows_in, weight):
    return jnp.dot(rows_in, weight, preferred_element_type=jnp.float32)


def flipped(index, mask):
    bit = 1
    while bit <= mask:
        if mask & bit:
            index = index + bit * (1 - 2 * ((index // bit) % 2))
        bit *= 2
    return index


def window_kernel(
    shards,
    groups,
    rows,
    share,
    deter_ref,
    embedded_ref,
    living_ref,
    weight_ref,
    carried_ref,
    lows_ref,
    weight,
    gath,
    parts,
    stats,
    weight_sem,
    low_sem,
    send_sem,
    recv_sem,
    stat_send,
    stat_recv,
):
    me = lax.axis_index("mp")
    peers = {mask: flipped(me, mask) for mask in range(1, shards)}
    fetch = pltpu.make_async_copy(weight_ref, weight, weight_sem)
    fetch.start()
    barrier = pltpu.get_barrier_semaphore()
    for mask in range(1, shards):
        pl.semaphore_signal(
            barrier,
            inc=1,
            device_id={"mp": peers[mask]},
            device_id_type=pl.DeviceIdType.MESH,
        )
    bits = []
    bit = shards // 2
    while bit:
        bits.append(bit)
        bit //= 2
    orders = [bits, [bits[1], bits[0]] + bits[2:]]
    half = rows // 2
    masks = sorted(range(1, shards), key=lambda mask: (mask.bit_count(), mask))

    def source(mask):
        return me if mask == 0 else peers[mask]

    def hop(g, s, mask, via):
        block = gath.at[g, source(mask), pl.ds(s * half, half)]
        return pltpu.make_async_remote_copy(
            src_ref=block,
            dst_ref=block,
            send_sem=send_sem.at[g, s, mask ^ via],
            recv_sem=recv_sem.at[g, s, mask ^ via],
            device_id={"mp": peers[via]},
            device_id_type=pl.DeviceIdType.MESH,
        )

    def forward(g, s, mask):
        order = orders[s]
        last = max([order.index(bit) for bit in order if mask & bit], default=-1)
        for via in order[last + 1 :]:
            hop(g, s, mask, via).start()

    def arriving(g, s, mask):
        block = gath.at[g, source(mask), pl.ds(s * half, half)]
        return pltpu.make_async_remote_copy(
            src_ref=block,
            dst_ref=block,
            send_sem=send_sem.at[g, s, mask],
            recv_sem=recv_sem.at[g, s, mask],
            device_id={"mp": peers[mask]},
            device_id_type=pl.DeviceIdType.MESH,
        )

    def launch(g):
        here = pl.ds(g * rows, rows)
        gath[g, me] = carried_ref[here, :].astype(jnp.bfloat16)
        for s in range(2):
            forward(g, s, 0)

    def stat_copy(g, mask):
        return pltpu.make_async_remote_copy(
            src_ref=stats.at[g, 0],
            dst_ref=stats.at[g, mask],
            send_sem=stat_send.at[g, mask],
            recv_sem=stat_recv.at[g, mask],
            device_id={"mp": peers[mask]},
            device_id_type=pl.DeviceIdType.MESH,
        )

    def multiply(g, rows_in, start, depth, first):
        for part in range(3):
            term = jnp.dot(
                rows_in, weight[part, pl.ds(start, depth), :], preferred_element_type=jnp.float32
            )
            if first:
                parts[g, part] = term
            else:
                parts[g, part] += term

    carried_ref[...] = deter_ref[...]
    pl.semaphore_wait(barrier, shards - 1)
    for g in range(groups):
        launch(g)
    fetch.wait()

    def step(t, _):
        for g in range(groups):
            seen = set()

            def need(s, mask):
                if (s, mask) not in seen:
                    seen.add((s, mask))
                    arriving(g, s, mask).wait_recv()
                    forward(g, s, mask)

            multiply(g, embedded_ref[t, pl.ds(g * rows, rows), :], 0, HID, True)
            for s in range(2):
                need(s, orders[s][0])
            for mask in [0] + masks:
                if mask:
                    for s in range(2):
                        need(s, mask)
                start = pl.multiple_of(HID + source(mask) * share, share)
                multiply(g, gath[g, source(mask)], start, share, False)
            keep = pltpu.make_async_copy(gath.at[g], lows_ref.at[t, g], low_sem)
            keep.start()
            sums = jnp.zeros((rows, 128), jnp.float32)
            squares = jnp.zeros((rows, 128), jnp.float32)
            for part in range(3):
                for column in range(0, share, 128):
                    piece = parts[g, part, :, pl.ds(column, 128)]
                    sums = sums + piece
                    squares = squares + piece * piece
            stats[g, 0, 0:1, :] = jnp.sum(sums.T, axis=0, keepdims=True)
            stats[g, 0, 1:2, :] = jnp.sum(squares.T, axis=0, keepdims=True)
            for s in range(2):
                for mask in masks:
                    arriving(g, s, mask).wait_send()
            keep.wait()
            for mask in masks:
                stat_copy(g, mask).start()
        for g in range(groups):
            for mask in masks:
                stat_copy(g, mask).wait()
            total = jnp.sum(stats[g], axis=0) / (3 * share * shards)
            average = jnp.broadcast_to(total[0:1], (128, rows)).T
            square = jnp.broadcast_to(total[1:2], (128, rows)).T
            inverse = lax.rsqrt(square - average * average + 1e-05)
            here = pl.ds(g * rows, rows)
            alive = living_ref[t, here, :]
            for column in range(0, share, 128):
                where = pl.ds(column, 128)
                normed = [(parts[g, part, :, where] - average) * inverse for part in range(3)]
                reset_gate = jax.nn.sigmoid(normed[0])
                candidate = jnp.tanh(reset_gate * normed[1])
                update = jax.nn.sigmoid(normed[2] - 1.0)
                before = carried_ref[here, where]
                renewed = update * candidate + (1.0 - update) * before
                carried_ref[here, where] = jnp.where(alive > 0, renewed, before)

            @pl.when(t < STEPS - 1)
            def _():
                launch(g)

        return 0

    lax.fori_loop(0, STEPS, step, 0)


def recurrence(deter, embedded, gate_weight, living, shards):
    rows_here, share = deter.shape
    groups = 2
    rows = rows_here // groups
    alive = jnp.broadcast_to(living[:, :, None], (STEPS, rows_here, 128))
    vmem = pl.BlockSpec(memory_space=pltpu.VMEM)
    hbm = pl.BlockSpec(memory_space=pl.ANY)
    dma = pltpu.SemaphoreType.DMA
    return pl.pallas_call(
        functools.partial(window_kernel, shards, groups, rows, share),
        out_shape=(
            jax.ShapeDtypeStruct((rows_here, share), jnp.float32),
            jax.ShapeDtypeStruct((STEPS, groups, shards, rows, share), jnp.bfloat16),
        ),
        in_specs=[vmem, vmem, vmem, hbm],
        out_specs=(vmem, hbm),
        scratch_shapes=[
            pltpu.VMEM(gate_weight.shape, jnp.bfloat16),
            pltpu.VMEM((groups, shards, rows, share), jnp.bfloat16),
            pltpu.VMEM((groups, 3, rows, share), jnp.float32),
            pltpu.VMEM((groups, shards, 2, rows), jnp.float32),
            dma,
            dma,
            dma((groups, 2, shards)),
            dma((groups, 2, shards)),
            dma((groups, shards)),
            dma((groups, shards)),
        ],
        compiler_params=pltpu.CompilerParams(
            collective_id=0, has_side_effects=True, vmem_limit_bytes=48 * 1024 * 1024
        ),
    )(deter, embedded, alive, gate_weight)


def spread_kernel(axis, count, block_ref, out_ref, send_sem, recv_sem):
    me = lax.axis_index(axis)
    barrier = pltpu.get_barrier_semaphore()
    for ahead in range(1, count):
        pl.semaphore_signal(
            barrier,
            inc=1,
            device_id={axis: (me + ahead) % count},
            device_id_type=pl.DeviceIdType.MESH,
        )
    pl.semaphore_wait(barrier, count - 1)

    def copy(ahead, slot):
        return pltpu.make_async_remote_copy(
            src_ref=block_ref,
            dst_ref=out_ref.at[slot],
            send_sem=send_sem.at[ahead],
            recv_sem=recv_sem.at[ahead],
            device_id={axis: (me + ahead) % count},
            device_id_type=pl.DeviceIdType.MESH,
        )

    for ahead in range(1, count):
        copy(ahead, me).start()
    out_ref[me] = block_ref[...]
    for ahead in range(1, count):
        copy(ahead, me).wait_send()
        copy(ahead, (me + count - ahead) % count).wait_recv()


def spread(block, axis, collective_id):
    count = lax.axis_size(axis)
    vmem = pl.BlockSpec(memory_space=pltpu.VMEM)
    return pl.pallas_call(
        functools.partial(spread_kernel, axis, count),
        out_shape=jax.ShapeDtypeStruct((count,) + block.shape, block.dtype),
        in_specs=[vmem],
        out_specs=vmem,
        scratch_shapes=[
            pltpu.SemaphoreType.DMA((count,)),
            pltpu.SemaphoreType.DMA((count,)),
        ],
        compiler_params=pltpu.CompilerParams(
            collective_id=collective_id, has_side_effects=True
        ),
    )(block)


def on_device(
    deter,
    draws,
    actions,
    horizons,
    offsets,
    embed_stoch,
    embed_act,
    gru_weight,
    prior_weight,
    logit_weight,
    head_weight,
):
    holders = lax.axis_size("task")
    device = lax.axis_index("task")
    shards = lax.axis_size("mp")
    shard_index = lax.axis_index("mp")
    rows_here, det_share = deter.shape
    block_rows = rows_here // BLK_DEV
    per_task = rows_here * holders // TASKS
    own_rows = rows_here // shards
    places = jnp.arange(holders, dtype=jnp.int32)
    classes = jnp.arange(CLASSES, dtype=jnp.int32)
    running = jnp.cumsum(offsets, axis=0) % holders
    packed = jnp.concatenate([draws, actions[:, None]], axis=1).astype(jnp.bfloat16)
    packed = spread(packed, "task", 1)
    packed = packed.reshape(holders, STEPS, GROUPS + 1, BLK_DEV, block_rows)
    at_slot = (device + running) % holders
    picked = places[:, None, None] == at_slot[None]
    packed = jnp.sum(
        jnp.where(picked[:, :, None, :, None], packed.astype(jnp.float32), 0.0), axis=0
    ).astype(jnp.int32)
    packed = packed.reshape(STEPS, GROUPS + 1, rows_here)
    draws_home = jnp.transpose(packed[:, :GROUPS], (0, 2, 1))
    hot = (draws_home[:, :, :, None] == classes).astype(jnp.bfloat16)
    hot = hot.reshape(STEPS * rows_here, GROUPS * CLASSES)
    action_hot = (
        packed[:, GROUPS].reshape(-1)[:, None] == jnp.arange(ACTS, dtype=jnp.int32)
    ).astype(jnp.bfloat16)
    embed_pre = product(hot, embed_stoch) + product(action_hot, embed_act)
    embedded = jax.nn.silu(normed_rows(embed_pre)).astype(jnp.bfloat16)
    embedded = embedded.reshape(STEPS, rows_here, HID)

    home_rows = device * rows_here + jnp.arange(rows_here, dtype=jnp.int32)
    task_ids = jnp.arange(TASKS, dtype=jnp.int32)
    horizon_rows = jnp.sum(
        jnp.where((home_rows // per_task)[:, None] == task_ids, horizons, 0), axis=1
    )
    alive = horizon_rows[None] > WSTART + jnp.arange(STEPS, dtype=jnp.int32)[:, None]
    living = alive.astype(jnp.float32)

    gate_weight = jnp.transpose(gru_weight, (1, 0, 2))
    carried, lows = recurrence(deter, embedded, gate_weight, living, shards)

    target = (device + running[-1]) % holders
    sending = places[:, None] == target[None, :]
    blocks = carried.reshape(BLK_DEV, block_rows, det_share)
    outgoing = jnp.where(sending[:, :, None, None], blocks[None], 0.0).astype(jnp.bfloat16)
    arrived = lax.all_to_all(
        outgoing.reshape(holders * BLK_DEV * block_rows, det_share),
        "task",
        split_axis=0,
        concat_axis=0,
        tiled=True,
    ).reshape(holders, BLK_DEV, block_rows, det_share)
    taking = places[:, None] == ((device - running[-1]) % holders)[None, :]
    final = jnp.sum(
        jnp.where(taking[:, :, None, None], arrived.astype(jnp.float32), 0.0), axis=0
    ).reshape(rows_here, det_share)

    def own(array, axis):
        return lax.dynamic_slice_in_dim(array, shard_index * own_rows, own_rows, axis)

    first = shard_index * own_rows
    group_rows = lows.shape[3]
    state_rows = lax.dynamic_slice(
        lows,
        (0, first // group_rows, 0, first % group_rows, 0),
        (STEPS, 1, shards, own_rows, det_share),
    )
    state_rows = jnp.transpose(state_rows, (0, 1, 3, 2, 4)).reshape(STEPS * own_rows, -1)
    hidden = jax.nn.silu(normed_rows(product(state_rows, prior_weight))).astype(jnp.bfloat16)
    raw = product(hidden, logit_weight).reshape(STEPS * own_rows, GROUPS, CLASSES)
    exponent = jnp.exp(5.0 * jnp.tanh(raw / 5.0))
    own_hot = own(draws_home, 1).reshape(STEPS * own_rows, GROUPS)[:, :, None] == classes
    chosen = jnp.sum(jnp.where(own_hot, exponent, 0.0), axis=-1)
    chances = 0.99 * chosen / jnp.sum(exponent, axis=-1) + 0.01 / CLASSES
    log_prob = jnp.sum(jnp.log(chances), axis=-1)
    head_out = product(hidden, head_weight)
    results = jnp.stack([log_prob, head_out[:, 0], jax.nn.sigmoid(head_out[:, 1])])
    results = results.reshape(3, STEPS, own_rows) * own(living, 1)[None]
    results = spread(results.reshape(3 * STEPS, own_rows), "mp", 2)
    results = spread(results, "task", 3)
    results = results.reshape(holders, shards, 3, STEPS, own_rows)
    results = jnp.transpose(results, (0, 2, 3, 1, 4)).reshape(
        holders, 3, STEPS, BLK_DEV, block_rows
    )
    source = (device - running) % holders
    from_home = places[:, None, None] == source[None]
    outs = jnp.sum(jnp.where(from_home[:, None, :, :, None], results, 0.0), axis=0)
    outs = outs.reshape(3, STEPS, rows_here)
    return (outs[0], outs[1], outs[2], final)


def solution(mesh):
    in_specs = (
        P("task", "mp"),
        P(None, None, "task"),
        P(None, "task"),
        P(),
        P(),
        P(),
        P(),
        P(None, None, "mp"),
        P(),
        P(),
        P(),
    )
    out_specs = (P(None, "task"), P(None, "task"), P(None, "task"), P("task", "mp"))
    return jax.shard_map(
        on_device, mesh=mesh, in_specs=in_specs, out_specs=out_specs, check_vma=False
    )
```
